32 devices in a mesh: groups: 2 (over y), sec: 4 (over z), blk: 4 (over x, core).
Axes of the slice: x: 2, y: 2, z: 4, core: 2. Of those that a mesh axis runs over, the one named last changes fastest.
Arguments:
- psi: bfloat16 [8, 4, 256, 256], P(('groups', 'sec'), 'blk'), parts along dimension 0, may hold values from -6 to 6
- own_env: bfloat16 [8, 4, 17, 256, 256], P(('groups', 'sec'), 'blk'), parts along dimension 0, may hold values from -0.375 to 0.375
- handoff_env: bfloat16 [8, 4, 17, 256, 256], P(('groups', 'sec'), 'blk'), parts along dimension 0, may hold values from -0.375 to 0.375
- sources: int32 [8, 4, 17], P(('groups', 'sec'), 'blk'), parts along dimension 0, may hold values from 0 to 3, as said below
Outputs:
- applied: bfloat16 [8, 4, 256, 256], P(('groups', 'sec'), 'blk'), parts along dimension 0
- rayleigh: float32 [8], P(('groups', 'sec')), parts along dimension 0
- residual_scale: float32 [8], P(('groups', 'sec')), parts along dimension 0
The draws below stay inside these ranges and needn't reach their ends.
There are 2 independent parts, one for each index of `groups`. The reference program is written for one: setup_inputs(seed, part) draws one part's arguments, and reference() takes and returns one part's arrays. A program takes and returns all parts, laid end to end along the dimension named above; each array names one. Nothing has to cross between parts.
Inputs may be any that keep to these rules, and one draw needn't show every extreme that they name: `sources`: every entry names a sector of the same section, and the 17 channels of each output sector name every one of the 4 sectors of its section.
All inputs are finite; a program needn't handle non-finite values.
Results may differ from the reference program's by a relative error of at most 0.0064.
Values may be sent and summed in bfloat16 or wider, within the bound.
No kernel may reach another device: no remote copies, remote signals or barrier semaphores. Data moves between devices by JAX's collectives and lax.ppermute only.
A program may use at most 64 MiB of HBM per device.

```python
import jax
import jax.numpy as jnp
from jax import lax

SB = 256
CH = 17
SEC_DEV = 1
SECTORS = 4
NSECT = 4


def draw_sources(key, part):
    blocks = SECTORS // SEC_DEV
    pairs = SEC_DEV * CH
    keys = jax.random.split(jax.random.fold_in(key, 11), NSECT * blocks)

    def single(subkey):
        first_key, second_key = jax.random.split(subkey)
        order = jax.random.permutation(first_key, blocks)
        offset = jax.random.randint(second_key, (), 0, SEC_DEV)
        slots = jnp.arange(pairs)
        device = order[slots % blocks]
        local = (slots // blocks + offset) % SEC_DEV
        return device * SEC_DEV + local
    table = jax.vmap(single)(keys)
    return table.reshape(NSECT, SECTORS, CH).astype(jnp.int32)


def levels(stream_key, dims, pieces, least, largest):
    gain = 1.0
    for dim, blocks in pieces:
        draws = jax.random.uniform(jax.random.fold_in(jax.random.fold_in(stream_key, 6), dim), (blocks,), jnp.float32, least / len(pieces), largest / len(pieces))
        gain = gain * jnp.repeat(jnp.exp(draws), dims[dim] // blocks).reshape((-1,) + (1,) * (len(dims) - 1 - dim))
    return gain


def centred(own_key, dims, deviation, most, pieces=(), kind=jnp.bfloat16):
    entries = deviation * jax.random.normal(own_key, dims, jnp.float32)
    if pieces:
        entries = entries * levels(own_key, dims, pieces, -0.22, 0.18)
    return jnp.clip(entries, -most, most).astype(kind)


def setup_inputs(seed: int = 0, part: int = 0) -> dict:
    key_list = jax.random.split(jax.random.key(seed), 5)
    own_keys = jax.random.split(jax.random.fold_in(key_list[4], part), 5)
    return {
        "psi": centred(own_keys[0], (NSECT, SECTORS, SB, SB), 1.0, 6.0, ((0, 4), (1, 4))),
        "own_env": centred(own_keys[1], (NSECT, SECTORS, CH, SB, SB), SB ** -0.5, 0.375, ((0, 4), (1, 4))),
        "handoff_env": centred(own_keys[2], (NSECT, SECTORS, CH, SB, SB), SB ** -0.5, 0.375, ((0, 4), (1, 4))),
        "sources": draw_sources(jax.random.fold_in(jax.random.fold_in(key_list[4], part), 71), part),
    }


def contract(picked, left, right):
    inner = jnp.einsum('qcab,qcbd->qcad', picked.astype(jnp.float32), right.astype(jnp.float32)).astype(jnp.bfloat16)
    return jnp.einsum('qcab,qcbd->qad', left.astype(jnp.float32), inner.astype(jnp.float32))

def section_step(item):
    vector, own, other, source, even = item
    left = jnp.where(even, own, other)
    right = jnp.where(even, other, own)
    first = contract(vector[source], left, right)
    widened = vector.astype(jnp.float32)
    along = jnp.sum(widened * first)
    mass = jnp.sum(widened * widened)
    alpha = along / mass
    resid = first - alpha * widened
    scale = jnp.sqrt(jnp.mean(resid * resid) + 1e-06)
    second = (resid / scale).astype(jnp.bfloat16)
    applied = contract(second[source], left, right).astype(jnp.bfloat16)
    return (applied, alpha, scale)

def reference(psi, own_env, handoff_env, sources):
    partner = handoff_env[jnp.arange(NSECT, dtype=jnp.int32) ^ 1]
    even = jnp.arange(NSECT, dtype=jnp.int32) % 2 == 0
    applied, alpha, scale = lax.map(section_step, (psi, own_env, partner, sources, even))
    return (applied, alpha, scale)
```

```python
import functools

import jax
import jax.numpy as jnp
from jax import lax
from jax.experimental import pallas as pl
from jax.experimental.pallas import tpu as pltpu
from jax.sharding import PartitionSpec as P

f32 = jnp.float32
bf16 = jnp.bfloat16
EXTRA = 16


def swap(value, axis, bit):
    return lax.ppermute(value, axis, [(i, i ^ bit) for i in range(lax.axis_size(axis))])


def dot(a, b):
    return jnp.dot(a, b, preferred_element_type=f32)


def stage_kernel(channels, psi, own, env, mass, sem):
    copies = [pltpu.make_async_copy(own.at[c], env.at[c], sem.at[c]) for c in range(channels)]
    for copy in copies:
        copy.start()
    for s in range(psi.shape[0]):
        wide = psi[s].astype(f32)
        total = jnp.sum(wide * wide, axis=(0, 1), keepdims=True)
        mass[s] = jnp.broadcast_to(total, mass.shape[1:])
    for copy in copies:
        copy.wait()


def first_kernel(channels, table, psi, own, partner, mass, env, parts, packed, sem):
    even = table[0] == 0
    me = table[1]
    copies = [pltpu.make_async_copy(partner.at[c], env.at[c], sem.at[c]) for c in range(channels)]
    for copy in copies:
        copy.start()
    parts[...] = jnp.zeros_like(parts)

    def body(left, right):
        for c in range(channels):
            source = table[2 + c]
            copies[c].wait()
            inner = dot(psi[source], right[c]).astype(bf16)
            parts[source] += dot(left[c], inner)

    @pl.when(even)
    def _():
        body(own, env)

    @pl.when(jnp.logical_not(even))
    def _():
        body(env, own)

    first = parts[0]
    for s in range(1, parts.shape[0]):
        first = first + parts[s]
    wide = psi[me].astype(f32)
    along = jnp.sum(wide * first, axis=(0, 1), keepdims=True)
    weight = mass[me][:1, :1]
    share = jnp.where(weight > 0, along / jnp.where(weight > 0, weight, 1.0), 0.0)
    rows = first.shape[0]
    packed[:rows] = (first - share * wide).astype(bf16)
    high = share.astype(bf16).astype(f32)
    middle = (share - high).astype(bf16).astype(f32)
    low = share - high - middle
    row = lax.broadcasted_iota(jnp.int32, (EXTRA, first.shape[1]), 0)
    tail = jnp.where(row == 0, high, jnp.where(row == 1, middle, jnp.where(row == 2, low, 0.0)))
    packed[rows:] = tail.astype(bf16)


def second_kernel(channels, table, vector, psi, own, env, mass, parts, applied, alpha_out, scale_out, total_ref):
    even = table[0] == 0
    width, rows, columns = parts.shape

    share, weight = [], []
    for m in range(width):
        bits = vector[m, rows:].astype(f32)
        share.append(bits[0:1, 0:1] + bits[1:2, 0:1] + bits[2:3, 0:1])
        weight.append(mass[m][:1, :1])
    along = share[0] * weight[0]
    whole = weight[0]
    for m in range(1, width):
        along += share[m] * weight[m]
        whole += weight[m]
    alpha = along / whole

    power = jnp.zeros((1, 1), f32)
    total = jnp.zeros((rows, columns), f32)
    for m in range(width):
        delta = share[m] - alpha
        resid = vector[m, :rows].astype(f32) + delta * psi[m].astype(f32)
        power += jnp.sum(resid * resid, axis=(0, 1), keepdims=True)
        total += delta * parts[m]
    scale = jnp.sqrt(power / (width * rows * columns) + 1e-06)
    total_ref[...] = total

    def body(left, right):
        summed = total_ref[...]
        for c in range(channels):
            summed += dot(left[c], dot(vector[table[2 + c], :rows], right[c]).astype(bf16))
        applied[...] = (summed / scale).astype(bf16)

    @pl.when(even)
    def _():
        body(own, env)

    @pl.when(jnp.logical_not(even))
    def _():
        body(env, own)

    alpha_out[0] = alpha[0, 0]
    scale_out[0] = scale[0, 0]


ANY = pl.BlockSpec(memory_space=pl.ANY)
VMEM = pl.BlockSpec(memory_space=pltpu.VMEM)
SMEM = pl.BlockSpec(memory_space=pltpu.SMEM)
PARAMS = pltpu.CompilerParams(vmem_limit_bytes=24 * 1024 * 1024)


def shards(psi, own_env, handoff_env, sources):
    partner = swap(handoff_env, "sec", 1)[0, 0]
    own = own_env[0, 0]
    channels, block = own.shape[0], own.shape[1:]
    width = lax.axis_size("blk")
    table = jnp.concatenate(
        [jnp.stack([lax.axis_index("sec") % 2, lax.axis_index("blk")]).astype(jnp.int32), sources[0, 0]]
    )
    psis = lax.all_gather(psi[0, 0], "blk", axis=0)
    envs = (channels,) + block
    held, mass = pl.pallas_call(
        functools.partial(stage_kernel, channels),
        in_specs=[VMEM, ANY],
        out_specs=[VMEM, VMEM],
        out_shape=[pltpu.VMEM(envs, bf16), pltpu.VMEM((width, 8, 128), f32)],
        scratch_shapes=[pltpu.SemaphoreType.DMA((channels,))],
        compiler_params=PARAMS,
        name="stage",
    )(psis, own)
    partner_held, parts, packed = pl.pallas_call(
        functools.partial(first_kernel, channels),
        in_specs=[SMEM, VMEM, VMEM, ANY, VMEM],
        out_specs=[VMEM, VMEM, VMEM],
        out_shape=[
            pltpu.VMEM(envs, bf16),
            pltpu.VMEM((width,) + block, f32),
            jax.ShapeDtypeStruct((block[0] + EXTRA, block[1]), bf16),
        ],
        scratch_shapes=[pltpu.SemaphoreType.DMA((channels,))],
        compiler_params=PARAMS,
        name="first",
    )(table, psis, held, partner, mass)
    vectors = lax.all_gather(packed, "blk", axis=0)
    applied, alpha, scale = pl.pallas_call(
        functools.partial(second_kernel, channels),
        in_specs=[SMEM, VMEM, VMEM, VMEM, VMEM, VMEM, VMEM],
        out_specs=[VMEM, SMEM, SMEM],
        out_shape=[
            jax.ShapeDtypeStruct(block, bf16),
            jax.ShapeDtypeStruct((1,), f32),
            jax.ShapeDtypeStruct((1,), f32),
        ],
        scratch_shapes=[pltpu.VMEM(block, f32)],
        compiler_params=PARAMS,
        name="second",
    )(table, vectors, psis, held, partner_held, mass, parts)
    return applied[None, None], alpha, scale


def solution(mesh):
    spec = P(("groups", "sec"), "blk")
    return jax.shard_map(
        shards,
        mesh=mesh,
        in_specs=(spec, spec, spec, spec),
        out_specs=(spec, P(("groups", "sec")), P(("groups", "sec"))),
        check_vma=False,
    )
```

```python
import functools

import jax
import jax.numpy as jnp
from jax import lax
from jax.experimental import pallas as pl
from jax.experimental.pallas import tpu as pltpu
from jax.sharding import PartitionSpec as P


f32 = jnp.float32
bf16 = jnp.bfloat16
EXTRA = 16
GROUP = 5

ANY = pl.BlockSpec(memory_space=pl.ANY)
HBM = pl.BlockSpec(memory_space=pltpu.HBM)
VMEM = pl.BlockSpec(memory_space=pltpu.VMEM)
SMEM = pl.BlockSpec(memory_space=pltpu.SMEM)
PARAMS = pltpu.CompilerParams(vmem_limit_bytes=16 * 1024 * 1024)


def swap(value, axis, bit):
    return lax.ppermute(value, axis, [(i, i ^ bit) for i in range(lax.axis_size(axis))])


def dot(a, b):
    return jnp.dot(a, b, preferred_element_type=f32)


def total_of(x):
    return jnp.sum(x, axis=(0, 1), keepdims=True)


def call(kernel, ins, outs, args, flops, aliases=None, scratch=()):
    return pl.pallas_call(
        kernel,
        in_specs=ins,
        out_specs=[spec for spec, _ in outs],
        out_shape=[shape for _, shape in outs],
        scratch_shapes=scratch,
        input_output_aliases=aliases or {},
        compiler_params=PARAMS,
        cost_estimate=pl.CostEstimate(flops=flops, transcendentals=0, bytes_accessed=0),
    )(*args)


def one_channel(table, psi, env, c):
    parity = table[0]
    source = table[2 + c]
    inner = dot(psi[source], env[1 - parity, c]).astype(bf16)
    return source, dot(env[parity, c], inner)


def opening_kernel(table, psi, own, chunk, env, parts, mass, order, starts, sem):
    copy = pltpu.make_async_copy(own, env.at[0], sem)
    copy.start()
    channels = own.shape[0]
    width = psi.shape[0]
    me = table[1]
    for k in range(chunk.shape[0]):
        env[1, k] = chunk[k]
    parts[...] = jnp.zeros_like(parts)
    for s in range(width):
        wide = psi[s].astype(f32)
        mass[s] = jnp.broadcast_to(total_of(wide * wide), mass.shape[1:])

    def by_source(m, place):
        starts[m] = place

        def look(c, at):
            order[at] = c
            return at + (table[2 + c] ^ me == m).astype(jnp.int32)

        return lax.fori_loop(0, channels, look, place)

    starts[width] = lax.fori_loop(0, width, by_source, 0)
    copy.wait()
    for k in range(chunk.shape[0]):
        source, product = one_channel(table, psi, env, k)
        parts[source] += product


def middle_kernel(base, table, psi, chunk, env_in, parts_in, env, parts, early, along):
    for k in range(chunk.shape[0]):
        env[1, base + k] = chunk[k]
    for k in range(chunk.shape[0]):
        source, product = one_channel(table, psi, env, base + k)
        parts[source] += product
    total = parts[0]
    for s in range(1, parts.shape[0]):
        total = total + parts[s]
    early[...] = total
    along[...] = jnp.broadcast_to(total_of(psi[table[1]].astype(f32) * total), along.shape)


def closing_kernel(base, table, psi, chunk, env_in, parts_in, early, along, mass, env, parts, packed):
    me = table[1]
    first = early[...]
    for k in range(chunk.shape[0]):
        env[1, base + k] = chunk[k]
    late = None
    for k in range(chunk.shape[0]):
        source, product = one_channel(table, psi, env, base + k)
        parts[source] += product
        late = product if late is None else late + product
    wide = psi[me].astype(f32)
    along_all = along[:1, :1] + total_of(wide * late)
    weight = mass[me][:1, :1]
    share = jnp.where(weight > 0, along_all / jnp.where(weight > 0, weight, 1.0), 0.0)
    rows, columns = first.shape
    packed[:rows] = (first + late - share * wide).astype(bf16)
    high = share.astype(bf16).astype(f32)
    middle = (share - high).astype(bf16).astype(f32)
    low = share - high - middle
    row = lax.broadcasted_iota(jnp.int32, (EXTRA, columns), 0)
    tail = jnp.where(row == 0, high, jnp.where(row == 1, middle, jnp.where(row == 2, low, 0.0)))
    packed[rows:] = tail.astype(bf16)


def second_kernel(low, high, more, width, table, order, starts, psi, env, *refs):
    count = high - low
    blocks, refs = refs[:count], refs[count:]
    if low:
        before, refs = refs[0], refs[1:]
    if high == width:
        (mass, parts), refs = refs[:2], refs[2:]
        stats_in, refs = refs[:more], refs[more:]
        applied, alpha_out, scale_out, summed, held = refs
    else:
        summed, stats, held = refs
    parity, me = table[0], table[1]
    rows, columns = psi.shape[1:]

    for k in range(count):
        held[k] = blocks[k][:rows]

    summed[...] = before[...] if low else jnp.zeros((rows, columns), f32)
    begin, end = starts[low], starts[high]

    def step(g, carry):
        total = None
        for k in range(GROUP):
            place = begin + g * GROUP + k
            valid = place < end
            c = order[jnp.where(valid, place, 0)]
            m = jnp.where(valid, (table[2 + c] ^ me) - low, 0)
            inner = jnp.where(valid, dot(held[m], env[1 - parity, c]), 0.0).astype(bf16)
            product = dot(env[parity, c], inner)
            total = product if total is None else total + product
        summed[...] += total
        return carry

    lax.fori_loop(0, (end - begin + GROUP - 1) // GROUP, step, 0)

    mine = []
    for k in range(count):
        bits = blocks[k][rows:].astype(f32)
        share = bits[0:1, 0:1] + bits[1:2, 0:1] + bits[2:3, 0:1]
        value = held[k].astype(f32)
        cross = total_of(value * psi[me ^ (low + k)].astype(f32))
        mine.append((share, total_of(value * value), cross))
    if high < width:
        for k in range(count):
            for j in range(3):
                stats[k, j] = jnp.broadcast_to(mine[k][j], stats.shape[2:])
        return

    triples = []
    for ref in stats_in:
        for k in range(ref.shape[0]):
            triples.append(tuple(ref[k, j][:1, :1] for j in range(3)))
    triples += mine
    along = jnp.zeros((1, 1), f32)
    whole = jnp.zeros((1, 1), f32)
    for m in range(width):
        weight = mass[me ^ m][:1, :1]
        along += triples[m][0] * weight
        whole += weight
    alpha = along / whole
    power = jnp.zeros((1, 1), f32)
    total = summed[...]
    for m in range(width):
        share, square, cross = triples[m]
        delta = share - alpha
        power += square + 2.0 * delta * cross + delta * delta * mass[me ^ m][:1, :1]
        total += delta * parts[me ^ m]
    scale = jnp.sqrt(power / (width * rows * columns) + 1e-06)
    applied[...] = (total / scale).astype(bf16)
    alpha_out[0] = alpha[0, 0]
    scale_out[0] = scale[0, 0]


def chunk_sizes(channels):
    return [2, channels - 6, 3, 1]


def shards(psi, own_env, handoff_env, sources):
    own, handoff = own_env[0, 0], handoff_env[0, 0]
    channels, block = own.shape[0], own.shape[1:]
    width = lax.axis_size("blk")
    work = 4 * block[0] ** 3
    sizes = chunk_sizes(channels)
    chunks, bases, base = [], [], 0
    for size in sizes:
        chunks.append(swap(handoff[base : base + size], "sec", 1))
        bases.append(base)
        base += size
    table = jnp.concatenate(
        [jnp.stack([lax.axis_index("sec") % 2, lax.axis_index("blk")]).astype(jnp.int32), sources[0, 0]]
    )
    psis = lax.all_gather(psi[0, 0], "blk", axis=0)

    env_shape = (VMEM, pltpu.VMEM((2, channels) + block, bf16))
    parts_shape = (VMEM, pltpu.VMEM((width,) + block, f32))
    tile = (8, 128)
    env, parts, mass, order, starts = call(
        opening_kernel,
        [SMEM, VMEM, HBM, VMEM],
        [
            env_shape,
            parts_shape,
            (VMEM, pltpu.VMEM((width,) + tile, f32)),
            (SMEM, jax.ShapeDtypeStruct((channels + 1,), jnp.int32)),
            (SMEM, jax.ShapeDtypeStruct((width + 1,), jnp.int32)),
        ],
        (table, psis, own, chunks[0]),
        work * sizes[0],
        scratch=[pltpu.SemaphoreType.DMA],
    )
    for k in range(1, len(sizes) - 1):
        env, parts, early, along = call(
            functools.partial(middle_kernel, bases[k]),
            [SMEM, VMEM, VMEM, VMEM, VMEM],
            [env_shape, parts_shape, (VMEM, pltpu.VMEM(block, f32)), (VMEM, pltpu.VMEM(tile, f32))],
            (table, psis, chunks[k], env, parts),
            work * sizes[k],
            aliases={3: 0, 4: 1},
        )
    env, parts, packed = call(
        functools.partial(closing_kernel, bases[-1]),
        [SMEM, VMEM, VMEM, VMEM, VMEM, VMEM, VMEM, VMEM],
        [env_shape, parts_shape, (VMEM, pltpu.VMEM((block[0] + EXTRA, block[1]), bf16))],
        (table, psis, chunks[-1], env, parts, early, along, mass),
        work * sizes[-1],
        aliases={3: 0, 4: 1},
    )

    blocks = {0: packed}
    bit = width // 2
    while bit:
        for m in sorted(blocks):
            blocks[m | bit] = swap(blocks[m], "blk", bit)
        bit //= 2

    cuts = sorted({0, min(2, width - 1), width - 1, width})
    summed, stats = None, []
    for low, high in zip(cuts[:-1], cuts[1:]):
        count = high - low
        last = high == width
        args = [table, order, starts, psis, env] + [blocks[m] for m in range(low, high)]
        specs = [SMEM, SMEM, SMEM, VMEM, VMEM] + [VMEM] * count
        if low:
            args.append(summed)
            specs.append(VMEM)
        scratch = [pltpu.VMEM((count,) + block, bf16)]
        if last:
            args += [mass, parts] + stats
            specs += [VMEM] * (2 + len(stats))
            outs = [
                (VMEM, jax.ShapeDtypeStruct(block, bf16)),
                (SMEM, jax.ShapeDtypeStruct((1,), f32)),
                (SMEM, jax.ShapeDtypeStruct((1,), f32)),
            ]
            scratch = [pltpu.VMEM(block, f32)] + scratch
        else:
            outs = [
                (VMEM, pltpu.VMEM(block, f32)),
                (VMEM, pltpu.VMEM((count, 3) + tile, f32)),
            ]
        result = call(
            functools.partial(second_kernel, low, high, len(stats), width),
            specs,
            outs,
            tuple(args),
            work * channels * count // width,
            scratch=scratch,
        )
        if not last:
            summed = result[0]
            stats.append(result[1])
    applied, alpha, scale = result
    return applied[None, None], alpha, scale


def solution(mesh):
    spec = P(("groups", "sec"), "blk")
    return jax.shard_map(
        shards,
        mesh=mesh,
        in_specs=(spec, spec, spec, spec),
        out_specs=(spec, P(("groups", "sec")), P(("groups", "sec"))),
        check_vma=False,
    )
```

```python
import functools

import jax
import jax.numpy as jnp
from jax import lax
from jax.experimental import pallas as pl
from jax.experimental.pallas import tpu as pltpu
from jax.sharding import PartitionSpec as P


f32 = jnp.float32
bf16 = jnp.bfloat16
EXTRA = 16
GROUP = 5

ANY = pl.BlockSpec(memory_space=pl.ANY)
HBM = pl.BlockSpec(memory_space=pltpu.HBM)
VMEM = pl.BlockSpec(memory_space=pltpu.VMEM)
SMEM = pl.BlockSpec(memory_space=pltpu.SMEM)
PARAMS = pltpu.CompilerParams(vmem_limit_bytes=16 * 1024 * 1024)


def swap(value, axis, bit):
    return lax.ppermute(value, axis, [(i, i ^ bit) for i in range(lax.axis_size(axis))])


def dot(a, b):
    return jnp.dot(a, b, preferred_element_type=f32)


def total_of(x):
    return jnp.sum(x, axis=(0, 1), keepdims=True)


def call(kernel, ins, outs, args, flops, aliases=None, scratch=()):
    return pl.pallas_call(
        kernel,
        in_specs=ins,
        out_specs=[spec for spec, _ in outs],
        out_shape=[shape for _, shape in outs],
        scratch_shapes=scratch,
        input_output_aliases=aliases or {},
        compiler_params=PARAMS,
        cost_estimate=pl.CostEstimate(flops=flops, transcendentals=0, bytes_accessed=0),
    )(*args)


def one_channel(table, psi, env, c):
    parity = table[0]
    source = table[2 + c]
    inner = dot(psi[source], env[1 - parity, c]).astype(bf16)
    return source, dot(env[parity, c], inner)


def cut_kernel(whole, piece, sem):
    copy = pltpu.make_async_copy(whole.at[pl.ds(0, piece.shape[0])], piece, sem)
    copy.start()
    copy.wait()


def opening_kernel(table, psi, own, chunk, env, parts, mass, order, starts, kept, sem):
    copy = pltpu.make_async_copy(own, env.at[0], sem)
    copy.start()
    channels = own.shape[0]
    width = psi.shape[0]
    me = table[1]
    for k in range(table.shape[0]):
        kept[k] = table[k]
    for k in range(chunk.shape[0]):
        env[1, k] = chunk[k]
    parts[...] = jnp.zeros_like(parts)
    for s in range(width):
        wide = psi[s].astype(f32)
        mass[s] = jnp.broadcast_to(total_of(wide * wide), mass.shape[1:])

    def by_source(m, place):
        starts[m] = place

        def look(c, at):
            order[at] = c
            return at + (table[2 + c] ^ me == m).astype(jnp.int32)

        return lax.fori_loop(0, channels, look, place)

    starts[width] = lax.fori_loop(0, width, by_source, 0)
    copy.wait()
    for k in range(chunk.shape[0]):
        source, product = one_channel(table, psi, env, k)
        parts[source] += product


def middle_kernel(base, table, psi, chunk, env_in, parts_in, env, parts, early, along):
    for k in range(chunk.shape[0]):
        env[1, base + k] = chunk[k]
    for k in range(chunk.shape[0]):
        source, product = one_channel(table, psi, env, base + k)
        parts[source] += product
    total = parts[0]
    for s in range(1, parts.shape[0]):
        total = total + parts[s]
    early[...] = total
    along[...] = jnp.broadcast_to(total_of(psi[table[1]].astype(f32) * total), along.shape)


def closing_kernel(base, table, psi, chunk, env_in, parts_in, early, along, mass, env, parts, packed):
    me = table[1]
    first = early[...]
    for k in range(chunk.shape[0]):
        env[1, base + k] = chunk[k]
    late = None
    for k in range(chunk.shape[0]):
        source, product = one_channel(table, psi, env, base + k)
        parts[source] += product
        late = product if late is None else late + product
    wide = psi[me].astype(f32)
    along_all = along[:1, :1] + total_of(wide * late)
    weight = mass[me][:1, :1]
    share = jnp.where(weight > 0, along_all / jnp.where(weight > 0, weight, 1.0), 0.0)
    rows, columns = first.shape
    packed[:rows] = (first + late - share * wide).astype(bf16)
    high = share.astype(bf16).astype(f32)
    middle = (share - high).astype(bf16).astype(f32)
    low = share - high - middle
    row = lax.broadcasted_iota(jnp.int32, (EXTRA, columns), 0)
    tail = jnp.where(row == 0, high, jnp.where(row == 1, middle, jnp.where(row == 2, low, 0.0)))
    packed[rows:] = tail.astype(bf16)


def gathered(table, order, psi_rows, env, blocks, held, low, begin, end):
    parity, me = table[0], table[1]
    lefts, inners = [], []
    for k in range(GROUP):
        valid = begin + k < end
        c = order[jnp.where(valid, begin + k, 0)]
        if len(blocks) > 1:
            vector = held[jnp.where(valid, (table[2 + c] ^ me) - low, 0)]
        else:
            vector = blocks[0][:psi_rows]
        inner = dot(vector, env[1 - parity, c])
        inners.append(jnp.where(valid, inner, 0.0).astype(bf16))
        lefts.append(env[parity, c])
    return dot(jnp.concatenate(lefts, axis=1), jnp.concatenate(inners, axis=0))


def own_sums(block, psi):
    rows = psi.shape[0]
    bits = block[rows:].astype(f32)
    share = bits[0:1, 0:1] + bits[1:2, 0:1] + bits[2:3, 0:1]
    value = block[:rows].astype(f32)
    return share, total_of(value * value), total_of(value * psi[...].astype(f32))


def second_kernel(low, high, table, order, starts, psi, env, *refs):
    count = high - low
    blocks, refs = refs[:count], refs[count:]
    if low:
        before, refs = refs[0], refs[1:]
    summed, stats, held = refs
    me = table[1]
    rows, columns = psi.shape[1:]
    if count > 1:
        for k in range(count):
            held[k] = blocks[k][:rows]
    summed[...] = before[...] if low else jnp.zeros((rows, columns), f32)
    begin, end = starts[low], starts[high]

    def step(g, carry):
        summed[...] += gathered(table, order, rows, env, blocks, held, low, begin + g * GROUP, end)
        return carry

    lax.fori_loop(0, (end - begin + GROUP - 1) // GROUP, step, 0)
    for k in range(count):
        for j, value in enumerate(own_sums(blocks[k], psi.at[me ^ (low + k)])):
            stats[k, j] = jnp.broadcast_to(value, stats.shape[2:])


def final_kernel(low, more, table, order, starts, psi, env, block, before, mass, parts, *refs):
    stats_in, refs = refs[:more], refs[more:]
    applied, alpha_out, scale_out, summed, ready, alpha_held, scale_held, sem = refs
    me = table[1]
    width, rows, columns = parts.shape
    begin, end = starts[low], starts[width]
    summed[...] = before[...]

    def step(g, carry):
        summed[...] += gathered(table, order, rows, env, [block], None, low, begin + g * GROUP, end)
        return carry

    lax.fori_loop(1, (end - begin + GROUP - 1) // GROUP, step, 0)

    triples = []
    for ref in stats_in:
        for k in range(ref.shape[0]):
            triples.append(tuple(ref[k, j][:1, :1] for j in range(3)))
    triples.append(own_sums(block, psi.at[me ^ low]))
    along = jnp.zeros((1, 1), f32)
    whole = jnp.zeros((1, 1), f32)
    for m in range(width):
        weight = mass[me ^ m][:1, :1]
        along += triples[m][0] * weight
        whole += weight
    alpha = along / whole
    power = jnp.zeros((1, 1), f32)
    total = summed[...]
    for m in range(width):
        share, square, cross = triples[m]
        delta = share - alpha
        power += square + 2.0 * delta * cross + delta * delta * mass[me ^ m][:1, :1]
        total += delta * parts[me ^ m]
    scale = jnp.sqrt(power / (width * rows * columns) + 1e-06)
    alpha_held[0] = alpha[0, 0]
    scale_held[0] = scale[0, 0]
    copies = [
        pltpu.make_async_copy(alpha_held, alpha_out, sem.at[0]),
        pltpu.make_async_copy(scale_held, scale_out, sem.at[1]),
        pltpu.make_async_copy(ready, applied, sem.at[2]),
    ]
    copies[0].start()
    copies[1].start()
    total += gathered(table, order, rows, env, [block], None, low, begin, end)
    ready[...] = (total / scale).astype(bf16)
    copies[2].start()
    for copy in copies:
        copy.wait()


def chunk_sizes(channels):
    return [2, channels - 6, 3, 1]


def shards(psi, own_env, handoff_env, sources):
    own, handoff = own_env[0, 0], handoff_env[0, 0]
    channels, block = own.shape[0], own.shape[1:]
    width = lax.axis_size("blk")
    work = 4 * block[0] ** 3
    sizes = chunk_sizes(channels)
    chunks, bases, base = [], [], 0
    for k, size in enumerate(sizes):
        if k == 0:
            (piece,) = call(
                cut_kernel,
                [HBM],
                [(VMEM, pltpu.VMEM((size,) + block, bf16))],
                (pltpu.with_memory_space_constraint(handoff, pltpu.HBM),),
                0,
                scratch=[pltpu.SemaphoreType.DMA],
            )
        else:
            piece = handoff[base : base + size]
        chunks.append(swap(piece, "sec", 1))
        bases.append(base)
        base += size
    table = jnp.concatenate(
        [jnp.stack([lax.axis_index("sec") % 2, lax.axis_index("blk")]).astype(jnp.int32), sources[0, 0]]
    )
    psis = lax.all_gather(psi[0, 0], "blk", axis=0)

    env_shape = (VMEM, pltpu.VMEM((2, channels) + block, bf16))
    parts_shape = (VMEM, pltpu.VMEM((width,) + block, f32))
    tile = (8, 128)
    env, parts, mass, order, starts, table = call(
        opening_kernel,
        [SMEM, VMEM, HBM, VMEM],
        [
            env_shape,
            parts_shape,
            (VMEM, pltpu.VMEM((width,) + tile, f32)),
            (SMEM, pltpu.SMEM((channels + 1,), jnp.int32)),
            (SMEM, pltpu.SMEM((width + 1,), jnp.int32)),
            (SMEM, pltpu.SMEM(table.shape, jnp.int32)),
        ],
        (table, psis, pltpu.with_memory_space_constraint(own, pltpu.HBM), chunks[0]),
        work * sizes[0],
        scratch=[pltpu.SemaphoreType.DMA],
    )
    for k in range(1, len(sizes) - 1):
        env, parts, early, along = call(
            functools.partial(middle_kernel, bases[k]),
            [SMEM, VMEM, VMEM, VMEM, VMEM],
            [env_shape, parts_shape, (VMEM, pltpu.VMEM(block, f32)), (VMEM, pltpu.VMEM(tile, f32))],
            (table, psis, chunks[k], env, parts),
            work * sizes[k],
            aliases={3: 0, 4: 1},
        )
    env, parts, packed = call(
        functools.partial(closing_kernel, bases[-1]),
        [SMEM, VMEM, VMEM, VMEM, VMEM, VMEM, VMEM, VMEM],
        [env_shape, parts_shape, (VMEM, pltpu.VMEM((block[0] + EXTRA, block[1]), bf16))],
        (table, psis, chunks[-1], env, parts, early, along, mass),
        work * sizes[-1],
        aliases={3: 0, 4: 1},
    )

    blocks = {0: packed}
    bit = width // 2
    while bit:
        for m in sorted(blocks):
            blocks[m | bit] = swap(blocks[m], "blk", bit)
        bit //= 2

    cuts = sorted({0, min(2, width - 1), width - 1})
    shared = [table, order, starts, psis, env]
    shared_specs = [SMEM, SMEM, SMEM, VMEM, VMEM]
    summed, stats = None, []
    for low, high in zip(cuts[:-1], cuts[1:]):
        count = high - low
        args = shared + [blocks[m] for m in range(low, high)] + ([summed] if low else [])
        summed, stat = call(
            functools.partial(second_kernel, low, high),
            shared_specs + [VMEM] * (len(args) - len(shared)),
            [(VMEM, pltpu.VMEM(block, f32)), (VMEM, pltpu.VMEM((count, 3) + tile, f32))],
            tuple(args),
            work * channels * count // width,
            scratch=[pltpu.VMEM((count,) + block, bf16)],
        )
        stats.append(stat)
    args = shared + [blocks[width - 1], summed, mass, parts] + stats
    applied, alpha, scale = call(
        functools.partial(final_kernel, width - 1, len(stats)),
        shared_specs + [VMEM] * (len(args) - len(shared)),
        [
            (HBM, jax.ShapeDtypeStruct(block, bf16)),
            (HBM, jax.ShapeDtypeStruct((1,), f32)),
            (HBM, jax.ShapeDtypeStruct((1,), f32)),
        ],
        tuple(args),
        work * channels // width,
        scratch=[
            pltpu.VMEM(block, f32),
            pltpu.VMEM(block, bf16),
            pltpu.SMEM((1,), f32),
            pltpu.SMEM((1,), f32),
            pltpu.SemaphoreType.DMA((3,)),
        ],
    )
    return applied[None, None], alpha, scale


def solution(mesh):
    spec = P(("groups", "sec"), "blk")
    return jax.shard_map(
        shards,
        mesh=mesh,
        in_specs=(spec, spec, spec, spec),
        out_specs=(spec, P(("groups", "sec")), P(("groups", "sec"))),
        check_vma=False,
    )
```

```python
import functools

import jax
import jax.numpy as jnp
from jax import lax
from jax.experimental import pallas as pl
from jax.experimental.pallas import tpu as pltpu
from jax.sharding import PartitionSpec as P


f32 = jnp.float32
bf16 = jnp.bfloat16
EXTRA = 8
GROUP = 5

ANY = pl.BlockSpec(memory_space=pl.ANY)
HBM = pl.BlockSpec(memory_space=pltpu.HBM)
VMEM = pl.BlockSpec(memory_space=pltpu.VMEM)
SMEM = pl.BlockSpec(memory_space=pltpu.SMEM)
PARAMS = pltpu.CompilerParams(vmem_limit_bytes=16 * 1024 * 1024)


def swap(value, axis, bit):
    return lax.ppermute(value, axis, [(i, i ^ bit) for i in range(lax.axis_size(axis))])


def dot(a, b):
    return jnp.dot(a, b, preferred_element_type=f32)


def total_of(x):
    return jnp.sum(x, axis=(0, 1), keepdims=True)


def call(kernel, ins, outs, args, flops, aliases=None, scratch=()):
    return pl.pallas_call(
        kernel,
        in_specs=ins,
        out_specs=[spec for spec, _ in outs],
        out_shape=[shape for _, shape in outs],
        scratch_shapes=scratch,
        input_output_aliases=aliases or {},
        compiler_params=PARAMS,
        cost_estimate=pl.CostEstimate(flops=flops, transcendentals=0, bytes_accessed=0),
    )(*args)


def one_channel(table, psi, env, c):
    parity = table[0]
    source = table[2 + c]
    inner = dot(psi[source], env[1 - parity, c]).astype(bf16)
    return source, dot(env[parity, c], inner)


def cut_kernel(base, whole, *refs):
    pieces, sem = refs[:-1], refs[-1]
    copies = []
    for k, piece in enumerate(pieces):
        size = piece.shape[0]
        copies.append(pltpu.make_async_copy(whole.at[pl.ds(base, size)], piece, sem.at[k]))
        base += size
    for copy in copies:
        copy.start()
    for copy in copies:
        copy.wait()


def opening_kernel(table, psi, own, chunk, env, parts, mass, order, starts, kept, sem):
    copy = pltpu.make_async_copy(own, env.at[0], sem)
    copy.start()
    channels = own.shape[0]
    width = psi.shape[0]
    me = table[1]
    for k in range(table.shape[0]):
        kept[k] = table[k]
    for k in range(chunk.shape[0]):
        env[1, k] = chunk[k]
    parts[...] = jnp.zeros_like(parts)
    for s in range(width):
        wide = psi[s].astype(f32)
        mass[s] = jnp.broadcast_to(total_of(wide * wide), mass.shape[1:])

    def by_source(m, place):
        starts[m] = place

        def look(c, at):
            order[at] = c
            return at + (table[2 + c] ^ me == m).astype(jnp.int32)

        return lax.fori_loop(0, channels, look, place)

    starts[width] = lax.fori_loop(0, width, by_source, 0)
    copy.wait()
    for k in range(chunk.shape[0]):
        source, product = one_channel(table, psi, env, k)
        parts[source] += product


def middle_kernel(base, table, psi, chunk, env_in, parts_in, env, parts, early, along):
    for k in range(chunk.shape[0]):
        env[1, base + k] = chunk[k]
    for k in range(chunk.shape[0]):
        source, product = one_channel(table, psi, env, base + k)
        parts[source] += product
    total = parts[0]
    for s in range(1, parts.shape[0]):
        total = total + parts[s]
    early[...] = total
    along[...] = jnp.broadcast_to(total_of(psi[table[1]].astype(f32) * total), along.shape)


def closing_kernel(base, table, psi, chunk, env_in, parts_in, early, along, mass, env, parts, packed):
    me = table[1]
    first = early[...]
    for k in range(chunk.shape[0]):
        env[1, base + k] = chunk[k]
    late = None
    for k in range(chunk.shape[0]):
        source, product = one_channel(table, psi, env, base + k)
        parts[source] += product
        late = product if late is None else late + product
    wide = psi[me].astype(f32)
    along_all = along[:1, :1] + total_of(wide * late)
    weight = mass[me][:1, :1]
    share = jnp.where(weight > 0, along_all / jnp.where(weight > 0, weight, 1.0), 0.0)
    rows, columns = first.shape
    packed[:rows] = (first + late - share * wide).astype(bf16)
    high = share.astype(bf16).astype(f32)
    middle = (share - high).astype(bf16).astype(f32)
    low = share - high - middle
    row = lax.broadcasted_iota(jnp.int32, (EXTRA, columns), 0)
    tail = jnp.where(row == 0, high, jnp.where(row == 1, middle, jnp.where(row == 2, low, 0.0)))
    packed[rows:] = tail.astype(bf16)


def gathered(table, order, psi_rows, env, blocks, held, low, begin, end):
    parity, me = table[0], table[1]
    lefts, inners = [], []
    for k in range(GROUP):
        valid = begin + k < end
        c = order[jnp.where(valid, begin + k, 0)]
        if len(blocks) > 1:
            vector = held[jnp.where(valid, (table[2 + c] ^ me) - low, 0)]
        else:
            vector = blocks[0][:psi_rows]
        inner = dot(vector, env[1 - parity, c])
        inners.append(jnp.where(valid, inner, 0.0).astype(bf16))
        lefts.append(env[parity, c])
    return dot(jnp.concatenate(lefts, axis=1), jnp.concatenate(inners, axis=0))


def own_sums(block, psi):
    rows = psi.shape[0]
    bits = block[rows:].astype(f32)
    share = bits[0:1, 0:1] + bits[1:2, 0:1] + bits[2:3, 0:1]
    value = block[:rows].astype(f32)
    return share, total_of(value * value), total_of(value * psi[...].astype(f32))


def second_kernel(low, high, table, order, starts, psi, env, *refs):
    count = high - low
    blocks, refs = refs[:count], refs[count:]
    if low:
        before, refs = refs[0], refs[1:]
    summed, stats, held = refs
    me = table[1]
    rows, columns = psi.shape[1:]
    if count > 1:
        for k in range(count):
            held[k] = blocks[k][:rows]
    summed[...] = before[...] if low else jnp.zeros((rows, columns), f32)
    begin, end = starts[low], starts[high]

    def step(g, carry):
        summed[...] += gathered(table, order, rows, env, blocks, held, low, begin + g * GROUP, end)
        return carry

    lax.fori_loop(0, (end - begin + GROUP - 1) // GROUP, step, 0)
    for k in range(count):
        for j, value in enumerate(own_sums(blocks[k], psi.at[me ^ (low + k)])):
            stats[k, j] = jnp.broadcast_to(value, stats.shape[2:])


def final_kernel(low, more, table, order, starts, psi, env, block, before, mass, parts, *refs):
    stats_in, refs = refs[:more], refs[more:]
    applied, alpha_out, scale_out, summed, ready, alpha_held, scale_held, sem = refs
    me = table[1]
    width, rows, columns = parts.shape
    begin, end = starts[low], starts[width]
    summed[...] = before[...]

    def step(g, carry):
        summed[...] += gathered(table, order, rows, env, [block], None, low, begin + g * GROUP, end)
        return carry

    lax.fori_loop(1, (end - begin + GROUP - 1) // GROUP, step, 0)

    triples = []
    for ref in stats_in:
        for k in range(ref.shape[0]):
            triples.append(tuple(ref[k, j][:1, :1] for j in range(3)))
    triples.append(own_sums(block, psi.at[me ^ low]))
    along = jnp.zeros((1, 1), f32)
    whole = jnp.zeros((1, 1), f32)
    for m in range(width):
        weight = mass[me ^ m][:1, :1]
        along += triples[m][0] * weight
        whole += weight
    alpha = along / whole
    power = jnp.zeros((1, 1), f32)
    total = summed[...]
    for m in range(width):
        share, square, cross = triples[m]
        delta = share - alpha
        power += square + 2.0 * delta * cross + delta * delta * mass[me ^ m][:1, :1]
        total += delta * parts[me ^ m]
    scale = jnp.sqrt(power / (width * rows * columns) + 1e-06)
    alpha_held[0] = alpha[0, 0]
    scale_held[0] = scale[0, 0]
    copies = [
        pltpu.make_async_copy(alpha_held, alpha_out, sem.at[0]),
        pltpu.make_async_copy(scale_held, scale_out, sem.at[1]),
        pltpu.make_async_copy(ready, applied, sem.at[2]),
    ]
    copies[0].start()
    copies[1].start()
    total += gathered(table, order, rows, env, [block], None, low, begin, end)
    ready[...] = (total / scale).astype(bf16)
    copies[2].start()
    for copy in copies:
        copy.wait()


def chunk_sizes(channels):
    return [2, channels - 3, 1]


def shards(psi, own_env, handoff_env, sources):
    own, handoff = own_env[0, 0], handoff_env[0, 0]
    channels, block = own.shape[0], own.shape[1:]
    width = lax.axis_size("blk")
    work = 4 * block[0] ** 3
    sizes = chunk_sizes(channels)
    bases = [sum(sizes[:k]) for k in range(len(sizes))]
    handoff = pltpu.with_memory_space_constraint(handoff, pltpu.HBM)
    pieces = []
    for low, high in ((0, 1), (1, len(sizes))):
        pieces += call(
            functools.partial(cut_kernel, bases[low]),
            [HBM],
            [(VMEM, pltpu.VMEM((size,) + block, bf16)) for size in sizes[low:high]],
            (handoff,),
            0,
            scratch=[pltpu.SemaphoreType.DMA((high - low,))],
        )
    chunks = []
    for piece in pieces:
        chunks.append(swap(piece, "sec", 1))
    table = jnp.concatenate(
        [jnp.stack([lax.axis_index("sec") % 2, lax.axis_index("blk")]).astype(jnp.int32), sources[0, 0]]
    )
    psis = lax.all_gather(psi[0, 0], "blk", axis=0)

    env_shape = (VMEM, pltpu.VMEM((2, channels) + block, bf16))
    parts_shape = (VMEM, pltpu.VMEM((width,) + block, f32))
    tile = (8, 128)
    env, parts, mass, order, starts, table = call(
        opening_kernel,
        [SMEM, VMEM, HBM, VMEM],
        [
            env_shape,
            parts_shape,
            (VMEM, pltpu.VMEM((width,) + tile, f32)),
            (SMEM, pltpu.SMEM((channels + 1,), jnp.int32)),
            (SMEM, pltpu.SMEM((width + 1,), jnp.int32)),
            (SMEM, pltpu.SMEM(table.shape, jnp.int32)),
        ],
        (table, psis, pltpu.with_memory_space_constraint(own, pltpu.HBM), chunks[0]),
        work * sizes[0],
        scratch=[pltpu.SemaphoreType.DMA],
    )
    for k in range(1, len(sizes) - 1):
        env, parts, early, along = call(
            functools.partial(middle_kernel, bases[k]),
            [SMEM, VMEM, VMEM, VMEM, VMEM],
            [env_shape, parts_shape, (VMEM, pltpu.VMEM(block, f32)), (VMEM, pltpu.VMEM(tile, f32))],
            (table, psis, chunks[k], env, parts),
            work * sizes[k],
            aliases={3: 0, 4: 1},
        )
    env, parts, packed = call(
        functools.partial(closing_kernel, bases[-1]),
        [SMEM, VMEM, VMEM, VMEM, VMEM, VMEM, VMEM, VMEM],
        [env_shape, parts_shape, (VMEM, pltpu.VMEM((block[0] + EXTRA, block[1]), bf16))],
        (table, psis, chunks[-1], env, parts, early, along, mass),
        work * sizes[-1],
        aliases={3: 0, 4: 1},
    )

    blocks = {0: packed}
    bit = width // 2
    while bit:
        for m in sorted(blocks):
            blocks[m | bit] = swap(blocks[m], "blk", bit)
        bit //= 2

    cuts = sorted({0, min(2, width - 1), width - 1})
    shared = [table, order, starts, psis, env]
    shared_specs = [SMEM, SMEM, SMEM, VMEM, VMEM]
    summed, stats = None, []
    for low, high in zip(cuts[:-1], cuts[1:]):
        count = high - low
        args = shared + [blocks[m] for m in range(low, high)] + ([summed] if low else [])
        summed, stat = call(
            functools.partial(second_kernel, low, high),
            shared_specs + [VMEM] * (len(args) - len(shared)),
            [(VMEM, pltpu.VMEM(block, f32)), (VMEM, pltpu.VMEM((count, 3) + tile, f32))],
            tuple(args),
            work * channels * count // width,
            scratch=[pltpu.VMEM((count,) + block, bf16)],
        )
        stats.append(stat)
    args = shared + [blocks[width - 1], summed, mass, parts] + stats
    applied, alpha, scale = call(
        functools.partial(final_kernel, width - 1, len(stats)),
        shared_specs + [VMEM] * (len(args) - len(shared)),
        [
            (HBM, jax.ShapeDtypeStruct(block, bf16)),
            (HBM, jax.ShapeDtypeStruct((1,), f32)),
            (HBM, jax.ShapeDtypeStruct((1,), f32)),
        ],
        tuple(args),
        work * channels // width,
        scratch=[
            pltpu.VMEM(block, f32),
            pltpu.VMEM(block, bf16),
            pltpu.SMEM((1,), f32),
            pltpu.SMEM((1,), f32),
            pltpu.SemaphoreType.DMA((3,)),
        ],
    )
    return applied[None, None], alpha, scale


def solution(mesh):
    spec = P(("groups", "sec"), "blk")
    return jax.shard_map(
        shards,
        mesh=mesh,
        in_specs=(spec, spec, spec, spec),
        out_specs=(spec, P(("groups", "sec")), P(("groups", "sec"))),
        check_vma=False,
    )
```

```python
import functools

import jax
import jax.numpy as jnp
from jax import lax
from jax.experimental import pallas as pl
from jax.experimental.pallas import tpu as pltpu
from jax.sharding import PartitionSpec as P


f32 = jnp.float32
bf16 = jnp.bfloat16
EXTRA = 8
GROUP = 5

ANY = pl.BlockSpec(memory_space=pl.ANY)
HBM = pl.BlockSpec(memory_space=pltpu.HBM)
VMEM = pl.BlockSpec(memory_space=pltpu.VMEM)
SMEM = pl.BlockSpec(memory_space=pltpu.SMEM)
PARAMS = pltpu.CompilerParams(vmem_limit_bytes=16 * 1024 * 1024)


def swap(value, axis, bit):
    return lax.ppermute(value, axis, [(i, i ^ bit) for i in range(lax.axis_size(axis))])


def dot(a, b):
    return jnp.dot(a, b, preferred_element_type=f32)


def total_of(x):
    return jnp.sum(x, axis=(0, 1), keepdims=True)


def call(kernel, ins, outs, args, flops, aliases=None, scratch=()):
    return pl.pallas_call(
        kernel,
        in_specs=ins,
        out_specs=[spec for spec, _ in outs],
        out_shape=[shape for _, shape in outs],
        scratch_shapes=scratch,
        input_output_aliases=aliases or {},
        compiler_params=PARAMS,
        cost_estimate=pl.CostEstimate(flops=flops, transcendentals=0, bytes_accessed=0),
    )(*args)


def one_channel(table, psi, env, c):
    parity = table[0]
    source = table[2 + c]
    inner = dot(psi[source], env[1 - parity, c]).astype(bf16)
    return source, dot(env[parity, c], inner)


def cut_kernel(base, whole, *refs):
    pieces, sem = refs[:-1], refs[-1]
    copies = []
    for k, piece in enumerate(pieces):
        size = piece.shape[0]
        copies.append(pltpu.make_async_copy(whole.at[pl.ds(base, size)], piece, sem.at[k]))
        base += size
    for copy in copies:
        copy.start()
    for copy in copies:
        copy.wait()


def opening_kernel(table, psi, own, chunk, env, parts, mass, order, starts, kept, sem):
    copy = pltpu.make_async_copy(own, env.at[0], sem)
    copy.start()
    channels = own.shape[0]
    width = psi.shape[0]
    me = table[1]
    for k in range(table.shape[0]):
        kept[k] = table[k]
    for k in range(chunk.shape[0]):
        env[1, k] = chunk[k]
    parts[...] = jnp.zeros_like(parts)
    for s in range(width):
        wide = psi[s].astype(f32)
        mass[s] = jnp.broadcast_to(total_of(wide * wide), mass.shape[1:])

    def by_source(m, place):
        starts[m] = place

        def look(c, at):
            order[at] = c
            return at + (table[2 + c] ^ me == m).astype(jnp.int32)

        return lax.fori_loop(0, channels, look, place)

    starts[width] = lax.fori_loop(0, width, by_source, 0)
    copy.wait()
    for k in range(chunk.shape[0]):
        source, product = one_channel(table, psi, env, k)
        parts[source] += product


def middle_kernel(base, table, psi, chunk, env_in, parts_in, env, parts, early, along):
    for k in range(chunk.shape[0]):
        env[1, base + k] = chunk[k]
    for k in range(chunk.shape[0]):
        source, product = one_channel(table, psi, env, base + k)
        parts[source] += product
    total = parts[0]
    for s in range(1, parts.shape[0]):
        total = total + parts[s]
    early[...] = total
    along[...] = jnp.broadcast_to(total_of(psi[table[1]].astype(f32) * total), along.shape)


def closing_kernel(base, table, psi, chunk, env_in, parts_in, early, along, mass, env, parts, packed):
    me = table[1]
    first = early[...]
    for k in range(chunk.shape[0]):
        env[1, base + k] = chunk[k]
    late = None
    for k in range(chunk.shape[0]):
        source, product = one_channel(table, psi, env, base + k)
        parts[source] += product
        late = product if late is None else late + product
    wide = psi[me].astype(f32)
    along_all = along[:1, :1] + total_of(wide * late)
    weight = mass[me][:1, :1]
    share = jnp.where(weight > 0, along_all / jnp.where(weight > 0, weight, 1.0), 0.0)
    rows, columns = first.shape
    packed[:rows] = (first + late - share * wide).astype(bf16)
    high = share.astype(bf16).astype(f32)
    middle = (share - high).astype(bf16).astype(f32)
    low = share - high - middle
    row = lax.broadcasted_iota(jnp.int32, (EXTRA, columns), 0)
    tail = jnp.where(row == 0, high, jnp.where(row == 1, middle, jnp.where(row == 2, low, 0.0)))
    packed[rows:] = tail.astype(bf16)


def gathered(table, order, psi_rows, env, blocks, held, low, begin, end):
    parity, me = table[0], table[1]
    lefts, inners = [], []
    for k in range(GROUP):
        valid = begin + k < end
        c = order[jnp.where(valid, begin + k, 0)]
        if len(blocks) > 1:
            vector = held[jnp.where(valid, (table[2 + c] ^ me) - low, 0)]
        else:
            vector = blocks[0][:psi_rows]
        inner = dot(vector, env[1 - parity, c])
        rounded = inner.astype(bf16)
        inners.append(jnp.where(valid, rounded, jnp.zeros_like(rounded)))
        lefts.append(env[parity, c])
    return dot(jnp.concatenate(lefts, axis=1), jnp.concatenate(inners, axis=0))


def own_sums(block, psi):
    rows = psi.shape[0]
    bits = block[rows:].astype(f32)
    share = bits[0:1, 0:1] + bits[1:2, 0:1] + bits[2:3, 0:1]
    value = block[:rows].astype(f32)
    return share, total_of(value * value), total_of(value * psi[...].astype(f32))


def second_kernel(low, high, table, order, starts, psi, env, *refs):
    count = high - low
    blocks, refs = refs[:count], refs[count:]
    if low:
        before, refs = refs[0], refs[1:]
    summed, stats, held = refs
    me = table[1]
    rows, columns = psi.shape[1:]
    if count > 1:
        for k in range(count):
            held[k] = blocks[k][:rows]
    summed[...] = before[...] if low else jnp.zeros((rows, columns), f32)
    begin, end = starts[low], starts[high]

    def step(g, carry):
        summed[...] += gathered(table, order, rows, env, blocks, held, low, begin + g * GROUP, end)
        return carry

    lax.fori_loop(0, (end - begin + GROUP - 1) // GROUP, step, 0)
    for k in range(count):
        for j, value in enumerate(own_sums(blocks[k], psi.at[me ^ (low + k)])):
            stats[k, j] = jnp.broadcast_to(value, stats.shape[2:])


def final_kernel(low, more, table, order, starts, psi, env, block, before, mass, parts, *refs):
    stats_in, refs = refs[:more], refs[more:]
    applied, alpha_out, scale_out, summed, ready, alpha_held, scale_held, sem = refs
    me = table[1]
    width, rows, columns = parts.shape
    begin, end = starts[low], starts[width]
    summed[...] = before[...]

    def step(g, carry):
        summed[...] += gathered(table, order, rows, env, [block], None, low, begin + g * GROUP, end)
        return carry

    lax.fori_loop(1, (end - begin + GROUP - 1) // GROUP, step, 0)

    triples = []
    for ref in stats_in:
        for k in range(ref.shape[0]):
            triples.append(tuple(ref[k, j][:1, :1] for j in range(3)))
    triples.append(own_sums(block, psi.at[me ^ low]))
    along = jnp.zeros((1, 1), f32)
    whole = jnp.zeros((1, 1), f32)
    for m in range(width):
        weight = mass[me ^ m][:1, :1]
        along += triples[m][0] * weight
        whole += weight
    alpha = along / whole
    power = jnp.zeros((1, 1), f32)
    total = summed[...]
    for m in range(width):
        share, square, cross = triples[m]
        delta = share - alpha
        power += square + 2.0 * delta * cross + delta * delta * mass[me ^ m][:1, :1]
        total += delta * parts[me ^ m]
    scale = jnp.sqrt(power / (width * rows * columns) + 1e-06)
    alpha_held[0] = alpha[0, 0]
    scale_held[0] = scale[0, 0]
    copies = [
        pltpu.make_async_copy(alpha_held, alpha_out, sem.at[0]),
        pltpu.make_async_copy(scale_held, scale_out, sem.at[1]),
        pltpu.make_async_copy(ready, applied, sem.at[2]),
    ]
    copies[0].start()
    copies[1].start()
    total += gathered(table, order, rows, env, [block], None, low, begin, end)
    ready[...] = (total / scale).astype(bf16)
    copies[2].start()
    for copy in copies:
        copy.wait()


def chunk_sizes(channels):
    return [2, channels - 3, 1]


def shards(psi, own_env, handoff_env, sources):
    own, handoff = own_env[0, 0], handoff_env[0, 0]
    channels, block = own.shape[0], own.shape[1:]
    width = lax.axis_size("blk")
    work = 4 * block[0] ** 3
    sizes = chunk_sizes(channels)
    bases = [sum(sizes[:k]) for k in range(len(sizes))]
    handoff = pltpu.with_memory_space_constraint(handoff, pltpu.HBM)
    pieces = []
    for low, high in ((0, 1), (1, len(sizes))):
        pieces += call(
            functools.partial(cut_kernel, bases[low]),
            [HBM],
            [(VMEM, pltpu.VMEM((size,) + block, bf16)) for size in sizes[low:high]],
            (handoff,),
            0,
            scratch=[pltpu.SemaphoreType.DMA((high - low,))],
        )
    chunks = []
    for piece in pieces:
        chunks.append(swap(piece, "sec", 1))
    table = jnp.concatenate(
        [jnp.stack([lax.axis_index("sec") % 2, lax.axis_index("blk")]).astype(jnp.int32), sources[0, 0]]
    )
    psis = lax.all_gather(psi[0, 0], "blk", axis=0)

    env_shape = (VMEM, pltpu.VMEM((2, channels) + block, bf16))
    parts_shape = (VMEM, pltpu.VMEM((width,) + block, f32))
    tile = (8, 128)
    env, parts, mass, order, starts, table = call(
        opening_kernel,
        [SMEM, VMEM, HBM, VMEM],
        [
            env_shape,
            parts_shape,
            (VMEM, pltpu.VMEM((width,) + tile, f32)),
            (SMEM, pltpu.SMEM((channels + 1,), jnp.int32)),
            (SMEM, pltpu.SMEM((width + 1,), jnp.int32)),
            (SMEM, pltpu.SMEM(table.shape, jnp.int32)),
        ],
        (table, psis, pltpu.with_memory_space_constraint(own, pltpu.HBM), chunks[0]),
        work * sizes[0],
        scratch=[pltpu.SemaphoreType.DMA],
    )
    for k in range(1, len(sizes) - 1):
        env, parts, early, along = call(
            functools.partial(middle_kernel, bases[k]),
            [SMEM, VMEM, VMEM, VMEM, VMEM],
            [env_shape, parts_shape, (VMEM, pltpu.VMEM(block, f32)), (VMEM, pltpu.VMEM(tile, f32))],
            (table, psis, chunks[k], env, parts),
            work * sizes[k],
            aliases={3: 0, 4: 1},
        )
    env, parts, packed = call(
        functools.partial(closing_kernel, bases[-1]),
        [SMEM, VMEM, VMEM, VMEM, VMEM, VMEM, VMEM, VMEM],
        [env_shape, parts_shape, (VMEM, pltpu.VMEM((block[0] + EXTRA, block[1]), bf16))],
        (table, psis, chunks[-1], env, parts, early, along, mass),
        work * sizes[-1],
        aliases={3: 0, 4: 1},
    )

    blocks = {0: packed}
    bit = width // 2
    while bit:
        for m in sorted(blocks):
            blocks[m | bit] = swap(blocks[m], "blk", bit)
        bit //= 2

    cuts = sorted({0, min(1, width - 1), min(2, width - 1), width - 1})
    shared = [table, order, starts, psis, env]
    shared_specs = [SMEM, SMEM, SMEM, VMEM, VMEM]
    summed, stats = None, []
    for low, high in zip(cuts[:-1], cuts[1:]):
        count = high - low
        args = shared + [blocks[m] for m in range(low, high)] + ([summed] if low else [])
        summed, stat = call(
            functools.partial(second_kernel, low, high),
            shared_specs + [VMEM] * (len(args) - len(shared)),
            [(VMEM, pltpu.VMEM(block, f32)), (VMEM, pltpu.VMEM((count, 3) + tile, f32))],
            tuple(args),
            work * channels * count // width,
            scratch=[pltpu.VMEM((count,) + block, bf16)],
        )
        stats.append(stat)
    args = shared + [blocks[width - 1], summed, mass, parts] + stats
    applied, alpha, scale = call(
        functools.partial(final_kernel, width - 1, len(stats)),
        shared_specs + [VMEM] * (len(args) - len(shared)),
        [
            (HBM, jax.ShapeDtypeStruct(block, bf16)),
            (HBM, jax.ShapeDtypeStruct((1,), f32)),
            (HBM, jax.ShapeDtypeStruct((1,), f32)),
        ],
        tuple(args),
        work * channels // width,
        scratch=[
            pltpu.VMEM(block, f32),
            pltpu.VMEM(block, bf16),
            pltpu.SMEM((1,), f32),
            pltpu.SMEM((1,), f32),
            pltpu.SemaphoreType.DMA((3,)),
        ],
    )
    return applied[None, None], alpha, scale


def solution(mesh):
    spec = P(("groups", "sec"), "blk")
    return jax.shard_map(
        shards,
        mesh=mesh,
        in_specs=(spec, spec, spec, spec),
        out_specs=(spec, P(("groups", "sec")), P(("groups", "sec"))),
        check_vma=False,
    )
```
